256 devices in a mesh: dp: 64 (over x, z, y_hi), expert: 4 (over y_lo, core).
Axes of the slice: x: 4, y: 4 (y_hi: 2, y_lo: 2; y = y_hi * 2 + y_lo), z: 8, core: 2. Of those that a mesh axis runs over, the one named last changes fastest.
Arguments:
- out_grad: bfloat16 [65536, 1024], P(('dp', 'expert')), may hold values from -6 to 6
- expert_of: int32 [65536, 1], P(('dp', 'expert')), may hold values from 0 to 3; in each aligned block of 256 rows (0 to 255, 256 to 511, ...) at most 128 rows name the same one
- pre_act: bfloat16 [131072, 4096], P(('dp', 'expert')), may hold values from -24 to 24
- down_weight: bfloat16 [4, 4096, 1024], P('expert', 'dp'), may hold values from -0.09375 to 0.09375
Outputs:
- pre_grad: bfloat16 [131072, 4096], P(('dp', 'expert'))
- weight_grad: float32 [4, 4096, 1024], P('expert', 'dp')
The draws below stay inside these ranges and needn't reach their ends.
Inputs may be any that keep to these rules, and one draw needn't show every extreme that they name: `expert_of`: within each aligned block of 256 rows (the rows of one device) no expert is named by more than 128 rows, and in some blocks one expert is named by exactly 128 rows.
All inputs are finite; a program needn't handle non-finite values.
Results may differ from the reference program's by a relative error of at most 0.0026.
Values may be sent and summed in bfloat16 or wider, within the bound.
No kernel may reach another device: no remote copies, remote signals or barrier semaphores. Data moves between devices by JAX's collectives and lax.ppermute only.
A program may use at most 128 MiB of HBM per device.

```python
import math
import jax
import jax.numpy as jnp
import numpy as np
from jax import lax

D = 1024
FF = 4096
TOK_DEV = 256
CAP = 128
EXPERTS = 4
TOKENS = 65536
ROWS = 131072
N_DP = 64
N_EXPERT = 4


def raised(array, stream_key, source, target, parts, factor):
    def block_of(dim):
        return (jnp.arange(array.shape[dim]) // (array.shape[dim] // parts)).reshape((-1,) + (1,) * (array.ndim - 1 - dim))

    one_side = jax.random.permutation(stream_key, parts)[block_of(target)]
    far = (block_of(target) + parts // 2) % parts
    return jnp.where((block_of(source) == one_side) | (block_of(source) == far), factor * array, array)


def block_levels(rng, shape, shards, smallest, largest):
    def one(dim, blocks):
        draws = jax.random.uniform(jax.random.fold_in(jax.random.fold_in(rng, 6), dim), (blocks,), jnp.float32, smallest / len(shards), largest / len(shards))
        return jnp.repeat(jnp.exp(draws), shape[dim] // blocks).reshape((-1,) + (1,) * (len(shape) - dim - 1))

    loudness = one(*shards[0])
    for cut in shards[1:]:
        loudness = loudness * one(*cut)
    return loudness


def routed_block(own_key, own, number, rows, count, top, most, skew):
    sequence = jax.random.permutation(own_key, count)
    heavy_load, usual = shares(count, rows * top, most, skew, True), shares(count, rows * top, most, skew, False)
    places = jnp.arange(count)

    def named(tallies, turn):
        used = int((tallies > 0).sum())
        fixed = max(1, used // 4)
        shifted = fixed + (places - fixed + turn * (used - fixed)) % max(1, count - fixed)
        return jnp.zeros((count,), jnp.int32).at[sequence[jnp.where(places < fixed, places, shifted)]].set(jnp.asarray(tallies, jnp.int32))

    tallies = jnp.where(number % 4 == 0, named(heavy_load, number // 4), named(usual, number - number // 4 - 1))
    mixed = jax.random.permutation(jax.random.fold_in(own, 3), count)
    source_of, taker = mixed[0:count // 2 * 2:2], mixed[1:count // 2 * 2:2]
    slack = jnp.minimum(tallies[source_of] - 1, most - tallies[taker]) // 2
    slack = jnp.where((source_of == sequence[0]) | (taker == sequence[0]) | (tallies[taker] == 0), 0, jnp.maximum(slack, 0))
    shifted = jax.random.randint(jax.random.fold_in(own, 4), (count // 2,), 0, 1 << 20) % (slack + 1)
    tallies = tallies.at[source_of].add(-shifted).at[taker].add(shifted)
    labels = jnp.searchsorted(jnp.cumsum(tallies), jnp.arange(rows * top), side="right").astype(jnp.int32)
    grid = labels.reshape(top, rows).T
    grid = grid[jax.random.permutation(jax.random.fold_in(own, 1), rows)]
    turn = jax.random.randint(jax.random.fold_in(own, 2), (rows, 1), 0, top)
    return jnp.take_along_axis(grid, (jnp.arange(top)[None, :] + turn) % top, axis=1)


def shares(count, total, reach, lean, full):
    portions = [(1 << 20) // math.isqrt(rank ** lean) + 1 for rank in range(1, count + 1)]
    largest = reach if full else min(reach, max(-(-total // count), total * portions[0] // sum(portions)))
    least = 1 if total - largest >= count - 1 else 0
    counts, rest = [largest] + [least] * (count - 1), total - largest - least * (count - 1)
    while rest > 0:
        movable = [i for i in range(1, count) if counts[i] < largest] or [i for i in range(1, count) if counts[i] < reach]
        mass, budget = sum([portions[i] for i in movable]), rest
        for i in movable:
            addition = min(reach - counts[i], max(1, budget * portions[i] // mass), rest)
            counts[i] = counts[i] + addition
            rest = rest - addition
    return np.array(counts)


def gaussian(stream_key, shape, deviation, reach, cuts=(), kind=jnp.bfloat16):
    array = deviation * jax.random.normal(stream_key, shape, jnp.float32)
    if cuts:
        array = array * block_levels(stream_key, shape, cuts, -0.22, 0.18)
    return jnp.clip(array, -reach, reach).astype(kind)


def noise_with(stream_key, dims, deviation, limit, pieces, heavy, kind=jnp.bfloat16):
    values = deviation * jax.random.normal(stream_key, dims, jnp.float32)
    if pieces:
        values = values * block_levels(stream_key, dims, pieces, -0.22, 0.18)
    return jnp.clip(raised(values, jax.random.fold_in(stream_key, 3), *heavy), -limit, limit).astype(kind)


def setup_inputs(seed: int = 0) -> dict:
    keys = jax.random.split(jax.random.key(seed), 5)
    out_grad = gaussian(keys[0], (TOKENS, D), 1.0, 6.0, ((0, 256),))
    expert_of_keys = jax.random.split(jax.random.fold_in(keys[1], 1), TOKENS // TOK_DEV)
    expert_of_turns = jax.random.permutation(jax.random.fold_in(keys[1], 3), TOKENS // TOK_DEV)
    expert_of = jax.vmap(lambda own, number: routed_block(jax.random.fold_in(keys[1], 2), own, number, TOK_DEV, EXPERTS, 1, CAP, 0))(expert_of_keys, expert_of_turns).reshape((TOKENS, 1))
    pre_act = noise_with(keys[2], (ROWS, FF), 1.0, 24.0, ((0, 256),), (0, 1, 256, 6.0))
    down_weight = gaussian(keys[3], (EXPERTS, FF, D), FF ** -0.5, 0.09375, ((0, 4), (1, 64)))
    return dict(out_grad=out_grad, expert_of=expert_of, pre_act=pre_act, down_weight=down_weight)


tanh_scale = 0.7978845608028654
cubic_weight = 0.044715

def activate(values):
    argument = tanh_scale * (values + cubic_weight * values * values * values)
    return 0.5 * values * (1.0 + jnp.tanh(argument))

def derivative(values):
    tangent = jnp.tanh(tanh_scale * (values + cubic_weight * values * values * values))
    return 0.5 * (1.0 + tangent) + 0.5 * values * (1.0 - tangent * tangent) * tanh_scale * (1.0 + 3.0 * cubic_weight * values * values)

def reference(out_grad, expert_of, pre_act, down_weight):
    blocks = N_DP * N_EXPERT
    routed = expert_of[:, 0].reshape(blocks, TOK_DEV)
    onehot = (routed[:, :, None] == jnp.arange(EXPERTS, dtype=jnp.int32)[None, None, :]).astype(jnp.int32)
    position = lax.optimization_barrier(jnp.sum((jnp.cumsum(onehot, axis=1) - onehot) * onehot, axis=2))
    block_id = jnp.arange(blocks, dtype=jnp.int32)[:, None]
    replica = block_id // N_EXPERT
    source = block_id % N_EXPERT
    target = ((replica * EXPERTS + routed) * N_EXPERT + source) * CAP + position
    dispatched = jnp.zeros((ROWS, D), jnp.bfloat16).at[target.reshape(-1).astype(jnp.int32)].set(out_grad)
    grads_in = dispatched.reshape(N_DP, EXPERTS, N_EXPERT * CAP, D)
    pre_in = pre_act.reshape(N_DP, EXPERTS, N_EXPERT * CAP, FF)
    weights32 = down_weight.astype(jnp.float32)

    def accumulate(running, inputs):
        arrived, pre_rows = inputs
        pre32 = pre_rows.astype(jnp.float32)
        arrived32 = arrived.astype(jnp.float32)
        hidden_grad = jnp.einsum('erd,efd->erf', arrived32, weights32)
        pre_grad = (hidden_grad * derivative(pre32)).astype(jnp.bfloat16)
        hidden = activate(pre32).astype(jnp.bfloat16)
        partial_value = jnp.einsum('erf,erd->efd', hidden.astype(jnp.float32), arrived32)
        return (running + partial_value, pre_grad)
    running, pre_grads = lax.scan(accumulate, jnp.zeros((EXPERTS, FF, D), jnp.float32), (grads_in, pre_in))
    factor = jnp.float32(1.0 / math.sqrt(N_DP * TOK_DEV))
    return (pre_grads.reshape(ROWS, FF), running * factor)
```

```python
import functools
import math

import jax
import jax.numpy as jnp
from jax import lax
from jax.experimental import pallas as pl
from jax.experimental.pallas import tpu as pltpu
from jax.sharding import Mesh
from jax.sharding import PartitionSpec as P


X, Z, Y, E = "dp_0", "dp_1", "dp_2", "expert"
DP = (X, Z, Y)
DP_EXPERT = (X, Z, Y, E)

tanh_scale = 0.7978845608028654
cubic_weight = 0.044715

VMEM = pltpu.VMEM
SMEM = pltpu.SMEM


def activate(values):
    argument = tanh_scale * (values + cubic_weight * values * values * values)
    return 0.5 * values * (1.0 + jnp.tanh(argument))


def derivative(values):
    square = values * values
    tangent = jnp.tanh(tanh_scale * (values + cubic_weight * square * values))
    return 0.5 * (1.0 + tangent) + 0.5 * values * (1.0 - tangent * tangent) * tanh_scale * (
        1.0 + 3.0 * cubic_weight * square
    )


def shift(value, axis, step):
    count = lax.axis_size(axis)
    return lax.ppermute(value, axis, [(i, (i + step) % count) for i in range(count)])


def swap(value, axis, mask):
    count = lax.axis_size(axis)
    return lax.ppermute(value, axis, [(i, i ^ mask) for i in range(count)])


def cost(flops, moved, tanhs=0):
    return pl.CostEstimate(flops=flops, bytes_accessed=moved, transcendentals=tanhs)


def dispatch_kernel(place, route_ref, token_ref, *outs):
    tokens = token_ref.shape[0]
    capacity = outs[0].shape[0]
    route = route_ref[...]
    named = lax.broadcasted_iota(jnp.int32, (8, tokens), 0) == route
    named = jnp.where(named, 1.0, 0.0)
    before = lax.broadcasted_iota(jnp.int32, (tokens, tokens), 0) < lax.broadcasted_iota(
        jnp.int32, (tokens, tokens), 1
    )
    counts = jnp.dot(
        named.astype(jnp.bfloat16),
        jnp.where(before, 1.0, 0.0).astype(jnp.bfloat16),
        preferred_element_type=jnp.float32,
    )
    slot = jnp.sum(counts * named, axis=0, keepdims=True).astype(jnp.int32)
    rows = lax.broadcasted_iota(jnp.int32, (capacity, tokens), 0)
    for mask, out in enumerate(outs):
        goal = place[0] ^ mask
        chosen = (rows == slot) & (route == goal)
        out[...] = jnp.dot(
            jnp.where(chosen, 1.0, 0.0).astype(jnp.bfloat16),
            token_ref[...],
            preferred_element_type=jnp.float32,
        ).astype(jnp.bfloat16)


def dispatch(place, route, tokens, experts):
    count, width = tokens.shape
    shape = jax.ShapeDtypeStruct((count // 2, width), jnp.bfloat16)
    return pl.pallas_call(
        dispatch_kernel,
        out_shape=(shape,) * experts,
        in_specs=[
            pl.BlockSpec(memory_space=SMEM),
            pl.BlockSpec(memory_space=VMEM),
            pl.BlockSpec(memory_space=VMEM),
        ],
        out_specs=(pl.BlockSpec(memory_space=VMEM),) * experts,
        cost_estimate=cost(2 * experts * (count // 2) * count * width, 6 * count * width),
        name="dispatch",
    )(place, route, tokens)


def collect_kernel(place, *refs):
    *pieces, out = refs
    rows = pieces[0].shape[0]
    for mask, piece in enumerate(pieces):
        start = pl.multiple_of((place[0] ^ mask) * rows, rows)
        out[pl.ds(start, rows), :] = piece[...]


def collect(place, pieces):
    rows, width = pieces[0].shape
    return pl.pallas_call(
        collect_kernel,
        out_shape=jax.ShapeDtypeStruct((rows * len(pieces), width), jnp.bfloat16),
        in_specs=[pl.BlockSpec(memory_space=SMEM)] + [pl.BlockSpec(memory_space=VMEM)] * len(pieces),
        out_specs=pl.BlockSpec(memory_space=VMEM),
        cost_estimate=cost(0, 4 * rows * len(pieces) * width),
        name="collect",
    )(place, *pieces)


def hidden_kernel(place, value_ref, out_ref):
    out_ref[...] = activate(value_ref[...].astype(jnp.float32)).astype(jnp.bfloat16)


def hidden_part(place, pre_act, step, parts):
    rows, columns = pre_act.shape
    width = columns // parts
    block = rows // 4
    return pl.pallas_call(
        hidden_kernel,
        out_shape=jax.ShapeDtypeStruct((rows, width), jnp.bfloat16),
        grid_spec=pltpu.PrefetchScalarGridSpec(
            num_scalar_prefetch=1,
            grid=(4,),
            in_specs=[pl.BlockSpec((block, width), lambda i, place: (i, lax.rem(place[1] + step, parts)))],
            out_specs=pl.BlockSpec((block, width), lambda i, place: (i, 0)),
        ),
        cost_estimate=cost(12 * rows * width, 4 * rows * width, rows * width),
        name="hidden",
    )(place, pre_act)


def weight_kernel(parts, place, *refs):
    count = (len(refs) - parts) // 2
    hidden, tokens, outs = refs[:count], refs[count : 2 * count], refs[2 * count :]
    width = outs[0].shape[0]
    for step in range(parts):
        start = pl.multiple_of(lax.rem(place[2] + step, parts) * width, width)
        total = None
        for left, right in zip(hidden, tokens):
            term = lax.dot_general(
                left[:, pl.ds(start, width)],
                right[...],
                (((0,), (0,)), ((), ())),
                preferred_element_type=jnp.float32,
            )
            total = term if total is None else total + term
        outs[step][...] = total


def weight_parts(place, hidden, tokens, parts):
    rows, width = hidden[0].shape
    model = tokens[0].shape[1]
    shape = jax.ShapeDtypeStruct((width // parts, model), jnp.float32)
    return pl.pallas_call(
        functools.partial(weight_kernel, parts),
        out_shape=(shape,) * parts,
        in_specs=[pl.BlockSpec(memory_space=SMEM)]
        + [pl.BlockSpec(memory_space=VMEM)] * (len(hidden) + len(tokens)),
        out_specs=(pl.BlockSpec(memory_space=VMEM),) * parts,
        cost_estimate=cost(
            2 * len(hidden) * rows * width * model,
            2 * len(hidden) * rows * (width + model) + 4 * width * model,
        ),
        name="weight_terms",
    )(place, *hidden, *tokens)


def pre_grad_kernel(place, token_ref, weight_ref, value_ref, *rest):
    out_ref = rest[-1]
    term = lax.dot_general(
        token_ref[...],
        weight_ref[...],
        (((1,), (1,)), ((), ())),
        preferred_element_type=jnp.float32,
    )
    out_ref[...] = (term * derivative(value_ref[...].astype(jnp.float32))).astype(jnp.bfloat16)


def pre_grad_part(place, tokens, weights, pre_act, out, step, first, sizes):
    count_x, count_z = sizes
    rows, columns = pre_act.shape
    width = columns // (count_x * count_z)
    blocks = weights.shape[0] // width
    model = tokens.shape[1]

    def column(i, place):
        return (0, lax.rem(place[1] + first + i, count_x) * count_z + lax.rem(place[2] + step, count_z))

    specs = [
        pl.BlockSpec((rows, model), lambda i, place: (0, 0)),
        pl.BlockSpec((width, model), lambda i, place: (i, 0)),
        pl.BlockSpec((rows, width), column),
    ]
    operands = [tokens, weights, pre_act]
    aliases = {}
    if out is not None:
        specs.append(pl.BlockSpec(memory_space=pl.ANY))
        operands.append(out)
        aliases = {4: 0}
    return pl.pallas_call(
        pre_grad_kernel,
        out_shape=jax.ShapeDtypeStruct((rows, columns), jnp.bfloat16),
        grid_spec=pltpu.PrefetchScalarGridSpec(
            num_scalar_prefetch=1,
            grid=(blocks,),
            in_specs=specs,
            out_specs=pl.BlockSpec((rows, width), column),
        ),
        input_output_aliases=aliases,
        cost_estimate=cost(
            2 * rows * width * blocks * model, 4 * rows * width * blocks, rows * width * blocks
        ),
        name="pre_grad",
    )(place, *operands)


def body(out_grad, expert_of, pre_act, down_weight):
    experts = lax.axis_size(E)
    count_x, count_z = lax.axis_size(X), lax.axis_size(Z)
    replicas = lax.axis_size(DP)
    token_count, model_width = out_grad.shape
    here_y = lax.axis_index(Y)
    place = jnp.stack([lax.axis_index(E), lax.axis_index(X), lax.axis_index(Z)]).astype(jnp.int32)
    weight = down_weight[0]
    own_rows = weight.shape[0]

    other = swap(weight, Y, 1)
    pair = jnp.concatenate(
        [jnp.where(here_y == 0, weight, other), jnp.where(here_y == 0, other, weight)], axis=0
    )
    below, above, across = shift(pair, X, 1), shift(pair, X, count_x - 1), shift(pair, X, 2)
    block = jnp.concatenate([pair, above, across, below], axis=0)

    quarter = [hidden_part(place, pre_act, step, count_x) for step in (2, 1, 3, 0)]
    hidden_across, hidden_below, hidden_above, hidden_own = (
        shift(quarter[0], X, 2),
        shift(quarter[1], X, 1),
        shift(quarter[2], X, count_x - 1),
        quarter[3],
    )

    sent = dispatch(place, expert_of.reshape(1, token_count), out_grad, experts)
    arrived = collect(
        place, [sent[0]] + [swap(piece, E, mask) for mask, piece in enumerate(sent) if mask]
    )
    tokens_below, tokens_above = shift(arrived, X, 1), shift(arrived, X, count_x - 1)
    half = arrived.shape[0] // 2
    tokens_across = jnp.concatenate(
        [shift(tokens_below[:half], X, 1), shift(tokens_above[half:], X, count_x - 1)], axis=0
    )

    sizes = (count_x, count_z)
    pre_grad = pre_grad_part(place, arrived, block, pre_act, None, 0, 0, sizes)
    up, down = block, block
    for step in range(1, count_z // 2):
        up, down = shift(up, Z, 1), shift(down, Z, count_z - 1)
        pre_grad = pre_grad_part(place, arrived, down, pre_act, pre_grad, step, 0, sizes)
        pre_grad = pre_grad_part(place, arrived, up, pre_act, pre_grad, count_z - step, 0, sizes)
    middle = block.shape[0] // 2
    far_up, far_down = shift(up[:middle], Z, 1), shift(down[middle:], Z, count_z - 1)
    pre_grad = pre_grad_part(place, arrived, far_up, pre_act, pre_grad, count_z // 2, 0, sizes)
    pre_grad = pre_grad_part(
        place, arrived, far_down, pre_act, pre_grad, count_z // 2, count_x // 2, sizes
    )

    ready, up, down = lax.optimization_barrier((place, up, down))
    parts = weight_parts(
        ready,
        [hidden_own, hidden_above, hidden_below, hidden_across],
        [arrived, tokens_above, tokens_below, tokens_across],
        count_z,
    )
    far = parts[count_z // 2]
    cut = far.shape[0] // 2
    rising, falling = shift(far[:cut], Z, 1), shift(far[cut:], Z, count_z - 1)
    for step in range(count_z // 2 - 1, 0, -1):
        mine, yours = parts[step], parts[count_z - step]
        if step == count_z // 2 - 1:
            mine = jnp.concatenate([mine[:cut] + rising, mine[cut:]], axis=0)
            yours = jnp.concatenate([yours[:cut], yours[cut:] + falling], axis=0)
        else:
            mine, yours = mine + rising, yours + falling
        rising, falling = shift(mine, Z, 1), shift(yours, Z, count_z - 1)
    summed = parts[0] + rising + falling
    give = lax.dynamic_slice_in_dim(summed, (1 - here_y) * own_rows, own_rows, 0)
    keep = lax.dynamic_slice_in_dim(summed, here_y * own_rows, own_rows, 0)
    factor = 1.0 / math.sqrt(replicas * token_count)
    grad = (keep + swap(give, Y, 1)) * factor
    return (pre_grad, grad.reshape(1, own_rows, model_width))


def solution(mesh):
    torus = Mesh(mesh.devices.reshape(4, 8, 2, mesh.shape["expert"]), DP_EXPERT)
    return jax.shard_map(
        body,
        mesh=torus,
        in_specs=(
            P(DP_EXPERT, None),
            P(DP_EXPERT, None),
            P(DP_EXPERT, None),
            P("expert", DP, None),
        ),
        out_specs=(P(DP_EXPERT, None), P("expert", DP, None)),
        check_vma=False,
    )
```

```python
import functools
import math

import jax
import jax.numpy as jnp
from jax import lax
from jax.experimental import pallas as pl
from jax.experimental.pallas import tpu as pltpu
from jax.sharding import Mesh
from jax.sharding import PartitionSpec as P


X, Z, Y, E = "dp_0", "dp_1", "dp_2", "expert"
DP = (X, Z, Y)
DP_EXPERT = (X, Z, Y, E)

EARLY = (2, 3, 4, 5, 6)
LATE = (7, 0, 1)

tanh_scale = 0.7978845608028654
cubic_weight = 0.044715

VMEM = pl.BlockSpec(memory_space=pltpu.VMEM)
SMEM = pl.BlockSpec(memory_space=pltpu.SMEM)
ANY = pl.BlockSpec(memory_space=pl.ANY)
GRANT = pltpu.CompilerParams(vmem_limit_bytes=12 << 20)


def activate(values):
    square = values * values
    tangent = jnp.tanh(values * (tanh_scale + tanh_scale * cubic_weight * square))
    half = 0.5 * values
    return half + half * tangent


def derivative(values):
    square = values * values
    tangent = jnp.tanh(values * (tanh_scale + tanh_scale * cubic_weight * square))
    rise = values * (0.5 * tanh_scale + 1.5 * tanh_scale * cubic_weight * square)
    return (0.5 + rise) + tangent * (0.5 - rise * tangent)


def shift(value, axis, step):
    count = lax.axis_size(axis)
    return lax.ppermute(value, axis, [(i, (i + step) % count) for i in range(count)])


def swap(value, axis, mask):
    count = lax.axis_size(axis)
    return lax.ppermute(value, axis, [(i, i ^ mask) for i in range(count)])


def cost(flops, moved, tanhs=0):
    return pl.CostEstimate(flops=flops, bytes_accessed=moved, transcendentals=tanhs)


def bf16(*shape):
    return jax.ShapeDtypeStruct(shape, jnp.bfloat16)


def f32(*shape):
    return jax.ShapeDtypeStruct(shape, jnp.float32)


def dispatch_kernel(place, route_ref, token_ref, *outs):
    tokens = token_ref.shape[0]
    capacity = outs[0].shape[0]
    route = route_ref[...]
    named = lax.broadcasted_iota(jnp.int32, (8, tokens), 0) == route
    named = jnp.where(named, 1.0, 0.0)
    before = lax.broadcasted_iota(jnp.int32, (tokens, tokens), 0) < lax.broadcasted_iota(
        jnp.int32, (tokens, tokens), 1
    )
    counts = jnp.dot(
        named.astype(jnp.bfloat16),
        jnp.where(before, 1.0, 0.0).astype(jnp.bfloat16),
        preferred_element_type=jnp.float32,
    )
    slot = jnp.sum(counts * named, axis=0, keepdims=True).astype(jnp.int32)
    rows = lax.broadcasted_iota(jnp.int32, (capacity, tokens), 0)
    for mask, out in enumerate(outs):
        goal = place[0] ^ mask
        chosen = (rows == slot) & (route == goal)
        out[...] = jnp.dot(
            jnp.where(chosen, 1.0, 0.0).astype(jnp.bfloat16),
            token_ref[...],
            preferred_element_type=jnp.float32,
        ).astype(jnp.bfloat16)


def dispatch(place, route, tokens, experts):
    count, width = tokens.shape
    return pl.pallas_call(
        dispatch_kernel,
        out_shape=(bf16(count // 2, width),) * experts,
        in_specs=[SMEM, VMEM, VMEM],
        out_specs=(VMEM,) * experts,
        compiler_params=GRANT,
        cost_estimate=cost(experts * count * count * width, 6 * count * width),
        name="dispatch",
    )(place, route, tokens)


def collect_kernel(place, *refs):
    *pieces, low, high = refs
    rows = pieces[0].shape[0]
    half = len(pieces) // 2
    for mask, piece in enumerate(pieces):
        source = place[0] ^ mask
        start = pl.multiple_of(lax.rem(source, half) * rows, rows)

        @pl.when(source < half)
        def _():
            low[pl.ds(start, rows), :] = piece[...]

        @pl.when(source >= half)
        def _():
            high[pl.ds(start, rows), :] = piece[...]


def collect(place, pieces):
    rows, width = pieces[0].shape
    half = rows * len(pieces) // 2
    return pl.pallas_call(
        collect_kernel,
        out_shape=(bf16(half, width),) * 2,
        in_specs=[SMEM] + [VMEM] * len(pieces),
        out_specs=(VMEM,) * 2,
        compiler_params=GRANT,
        cost_estimate=cost(4 * half * width, 8 * half * width),
        name="collect",
    )(place, *pieces)


def pile_kernel(*refs):
    *pieces, out = refs
    rows = pieces[0].shape[0]
    for n, piece in enumerate(pieces):
        out[n * rows : (n + 1) * rows, :] = piece[...]


def pile(pieces):
    rows, width = pieces[0].shape
    return pl.pallas_call(
        pile_kernel,
        out_shape=bf16(len(pieces) * rows, width),
        in_specs=[VMEM] * len(pieces),
        out_specs=VMEM,
        compiler_params=GRANT,
        cost_estimate=cost(len(pieces) * rows * width, 4 * len(pieces) * rows * width),
        name="pile",
    )(*pieces)


def spread_kernel(bit, place, mine, other, out, run):
    high = lax.rem(place[2] // bit, 2)
    for n in range(mine.shape[0] // run):
        start = 2 * n * run
        out[pl.ds(pl.multiple_of(start + high * run, run), run), :] = mine[n * run : (n + 1) * run, :]
        out[pl.ds(pl.multiple_of(start + (1 - high) * run, run), run), :] = other[
            n * run : (n + 1) * run, :
        ]


def spread(place, mine, other, bit, run):
    rows, width = mine.shape
    return pl.pallas_call(
        functools.partial(spread_kernel, bit, run=run),
        out_shape=bf16(2 * rows, width),
        in_specs=[SMEM, VMEM, VMEM],
        out_specs=VMEM,
        compiler_params=GRANT,
        cost_estimate=cost(4 * rows * width, 8 * rows * width),
        name="spread",
    )(place, mine, other)


def column_of(place, sizes, right, up, width):
    count_x, count_z = sizes
    owner = lax.rem(place[1] + right, count_x) * count_z + lax.rem(place[2] + up, count_z)
    return pl.multiple_of(owner * width, width)


def cut_kernel(sizes, rights, ups, width, place, whole, *refs):
    *outs, sems = refs
    copies = []
    for n, (right, out) in enumerate(zip(rights, outs)):
        for i, up in enumerate(ups):
            copies.append(
                pltpu.make_async_copy(
                    whole.at[:, pl.ds(column_of(place, sizes, right, up, width), width)],
                    out.at[:, pl.ds(i * width, width)],
                    sems.at[n, i],
                )
            )
    for copy in copies:
        copy.start()
    for copy in copies:
        copy.wait()


def cut(place, whole, rights, ups, sizes):
    rows, columns = whole.shape
    width = columns // (sizes[0] * sizes[1])
    return pl.pallas_call(
        functools.partial(cut_kernel, sizes, rights, ups, width),
        out_shape=(bf16(rows, len(ups) * width),) * len(rights),
        in_specs=[SMEM, pl.BlockSpec(memory_space=pltpu.HBM)],
        out_specs=(VMEM,) * len(rights),
        scratch_shapes=[pltpu.SemaphoreType.DMA((len(rights), len(ups)))],
        compiler_params=GRANT,
        cost_estimate=cost(rows * columns, 2 * rows * columns),
        name="cut",
    )(place, whole)


def join_kernel(sizes, ups, width, place, *refs):
    pieces, whole, sems = refs[: sizes[0]], refs[-2], refs[-1]
    copies = []
    for right, piece in enumerate(pieces):
        for i, up in enumerate(ups):
            copies.append(
                pltpu.make_async_copy(
                    piece.at[:, pl.ds(i * width, width)],
                    whole.at[:, pl.ds(column_of(place, sizes, right, up, width), width)],
                    sems.at[right, i],
                )
            )
    for copy in copies:
        copy.start()
    for copy in copies:
        copy.wait()


def join(place, pieces, whole, shape, ups, sizes):
    rows, columns = shape
    width = columns // (sizes[0] * sizes[1])
    aliased = whole is not None
    return pl.pallas_call(
        functools.partial(join_kernel, sizes, ups, width),
        out_shape=bf16(rows, columns),
        in_specs=[SMEM] + [VMEM] * len(pieces) + [ANY] * aliased,
        out_specs=ANY,
        scratch_shapes=[pltpu.SemaphoreType.DMA((sizes[0], len(ups)))],
        input_output_aliases={1 + len(pieces): 0} if aliased else {},
        compiler_params=GRANT,
        cost_estimate=cost(rows * columns, 2 * rows * columns),
        name="join",
    )(place, *pieces, *([whole] if aliased else []))


def hidden_kernel(*refs):
    half = len(refs) // 2
    for value, out in zip(refs[:half], refs[half:]):
        out[...] = activate(value[...].astype(jnp.float32)).astype(jnp.bfloat16).T


def hidden_of(values):
    rows, width = values[0].shape
    block = rows // 4
    return pl.pallas_call(
        hidden_kernel,
        out_shape=(bf16(width, rows),) * len(values),
        grid=(4,),
        in_specs=[pl.BlockSpec((block, width), lambda i: (i, 0))] * len(values),
        out_specs=(pl.BlockSpec((width, block), lambda i: (0, i)),) * len(values),
        compiler_params=GRANT,
        cost_estimate=cost(
            12 * rows * width * len(values),
            4 * rows * width * len(values),
            rows * width * len(values),
        ),
        name="hidden",
    )(*values)


def weight_kernel(count, begun, parts, place, *refs):
    hidden, tokens, rest = refs[:count], refs[count : 3 * count], refs[3 * count :]
    rows = tokens[0].shape[0]
    total = rest[0][...] if begun else None
    for n, right in enumerate(tokens):
        term = jnp.dot(
            hidden[n // 2][:, (n % 2) * rows : (n % 2 + 1) * rows],
            right[...],
            preferred_element_type=jnp.float32,
        )
        total = term if total is None else total + term
    if not parts:
        rest[begun][...] = total
        return
    give, keep, whole = rest[begun:]
    whole[...] = total
    run = give.shape[0] // parts
    for n in range(parts):
        goal = pl.ds(n * run, run)
        for out, side in ((keep, place[3]), (give, 1 - place[3])):
            start = pl.multiple_of((2 * n + side) * run, run)
            out[goal, :] = whole[pl.ds(start, run), :].astype(out.dtype)


def weight_terms(place, hidden, tokens, begun, parts):
    columns, rows = hidden[0].shape
    model = tokens[0][0].shape[1]
    block = model // 4
    shapes, scratch = [f32(columns, model)], []
    if parts:
        shapes = [bf16(columns // 2, model), f32(columns // 2, model)]
        scratch = [pltpu.VMEM((columns, block), jnp.float32)]
    flat = [part for two in tokens for part in two]
    return pl.pallas_call(
        functools.partial(weight_kernel, len(hidden), len(begun), parts),
        out_shape=shapes,
        grid=(4,),
        in_specs=[SMEM]
        + [pl.BlockSpec((columns, rows), lambda i: (0, 0))] * len(hidden)
        + [pl.BlockSpec((rows // 2, block), lambda i: (0, i))] * len(flat)
        + [pl.BlockSpec((columns, block), lambda i: (0, i))] * len(begun),
        out_specs=[pl.BlockSpec((shape.shape[0], block), lambda i: (0, i)) for shape in shapes],
        scratch_shapes=scratch,
        compiler_params=GRANT,
        cost_estimate=cost(
            2 * len(hidden) * rows * columns * model,
            2 * len(hidden) * rows * (columns + model) + 4 * columns * model,
        ),
        name="weight_terms",
    )(place, *hidden, *flat, *begun)


def mix_kernel(keep, given, *outs):
    rows = outs[0].shape[0]
    for n, out in enumerate(outs):
        part = slice(n * rows, (n + 1) * rows)
        out[...] = (keep[part, :] + given[part, :].astype(jnp.float32)).astype(out.dtype)


def mix(keep, given, types):
    rows, width = keep.shape
    return pl.pallas_call(
        mix_kernel,
        out_shape=[jax.ShapeDtypeStruct((rows // len(types), width), kind) for kind in types],
        in_specs=[VMEM] * 2,
        out_specs=[VMEM] * len(types),
        compiler_params=GRANT,
        cost_estimate=cost(rows * width, 8 * rows * width),
        name="mix",
    )(keep, given)


def pre_grad_kernel(count, count_z, ups, place, *refs):
    mine, other = refs[:2]
    tokens, values = refs[2 : 2 + 2 * count], refs[2 + 2 * count : 2 + 3 * count]
    outs, weights = refs[2 + 3 * count : -1], refs[-1]
    run = mine.shape[0] // count_z
    for i, up in enumerate(ups):
        start = pl.multiple_of(lax.rem(place[2] + up, count_z) * run, run)
        for side, source in ((place[3], mine), (1 - place[3], other)):
            goal = pl.multiple_of((2 * i + side) * run, run)
            weights[pl.ds(goal, run), :] = source[pl.ds(start, run), :]
    rows = tokens[0].shape[0]
    for n in range(count):

        @pl.loop(0, 2)
        def _(half):
            token = jnp.where(half == 0, tokens[2 * n][...], tokens[2 * n + 1][...])
            term = lax.dot_general(
                token, weights[...], (((1,), (1,)), ((), ())), preferred_element_type=jnp.float32
            )
            part = pl.ds(pl.multiple_of(half * rows, rows), rows)
            slope = derivative(values[n][part, :].astype(jnp.float32))
            outs[n][part, :] = (term * slope).astype(jnp.bfloat16)


def pre_grad_of(place, weights, tokens, values, count_z, ups):
    rows, width = values[0].shape
    model = weights[0].shape[1]
    count = len(values)
    flat = [part for two in tokens for part in two]
    return pl.pallas_call(
        functools.partial(pre_grad_kernel, count, count_z, ups),
        out_shape=(bf16(rows, width),) * count,
        in_specs=[SMEM] + [VMEM] * (2 + 3 * count),
        out_specs=(VMEM,) * count,
        scratch_shapes=[pltpu.VMEM((width, model), jnp.bfloat16)],
        compiler_params=GRANT,
        cost_estimate=cost(
            2 * count * rows * width * model,
            2 * count * rows * (2 * width + model) + 4 * weights[0].size,
            count * rows * width,
        ),
        name="pre_grad",
    )(place, *weights, *flat, *values)


def near_grad_kernel(count, parts, place, low, high, *refs):
    pieces, values = refs[:parts], refs[parts : parts + count]
    outs, weights = refs[parts + count : -1], refs[-1]
    run = pieces[0].shape[0] // (2 * count)
    rows = low.shape[0]
    for n in range(count):
        for i in range(parts):
            for side, start in ((place[3], n * run), (1 - place[3], (count + n) * run)):
                goal = pl.multiple_of((2 * i + side) * run, run)
                weights[pl.ds(goal, run), :] = pieces[i][start : start + run, :]

        @pl.loop(0, 2)
        def _(half):
            token = jnp.where(half == 0, low[...], high[...])
            term = lax.dot_general(
                token, weights[...], (((1,), (1,)), ((), ())), preferred_element_type=jnp.float32
            )
            part = pl.ds(pl.multiple_of(half * rows, rows), rows)
            slope = derivative(values[n][part, :].astype(jnp.float32))
            outs[n][part, :] = (term * slope).astype(jnp.bfloat16)


def near_grad_of(place, tokens, pieces, values):
    rows, width = values[0].shape
    model = pieces[0].shape[1]
    count = len(values)
    return pl.pallas_call(
        functools.partial(near_grad_kernel, count, len(pieces)),
        out_shape=(bf16(rows, width),) * count,
        in_specs=[SMEM] + [VMEM] * (2 + len(pieces) + count),
        out_specs=(VMEM,) * count,
        scratch_shapes=[pltpu.VMEM((width, model), jnp.bfloat16)],
        compiler_params=GRANT,
        cost_estimate=cost(
            2 * count * rows * width * model,
            2 * count * rows * 2 * width + 2 * len(pieces) * pieces[0].size,
            count * rows * width,
        ),
        name="near_grad",
    )(place, *tokens, *pieces, *values)


def sum_kernel(factor, own, *refs):
    *pieces, out = refs
    total = own[...]
    for piece in pieces:
        total = total + piece[...].astype(jnp.float32)
    out[...] = total * factor


def sum_of(own, pieces, factor):
    return pl.pallas_call(
        functools.partial(sum_kernel, factor),
        out_shape=f32(*own.shape),
        in_specs=[VMEM] * (1 + len(pieces)),
        out_specs=VMEM,
        compiler_params=GRANT,
        cost_estimate=cost(len(pieces) * own.size, 2 * len(pieces) * own.size + 8 * own.size),
        name="sum_terms",
    )(own, *pieces)


def body(out_grad, expert_of, pre_act, down_weight):
    experts = lax.axis_size(E)
    count_x, count_z = lax.axis_size(X), lax.axis_size(Z)
    sizes = (count_x, count_z)
    replicas = lax.axis_size(DP)
    token_count, model_width = out_grad.shape
    place = jnp.stack([lax.axis_index(axis) for axis in (E, X, Z, Y)]).astype(jnp.int32)
    weight = down_weight[0]
    own_rows = weight.shape[0]

    others = tuple(range(1, count_x))
    cuts = cut(place, pre_act, others, EARLY, sizes)
    early = list(cut(place, pre_act, (0,), EARLY, sizes))
    early += [shift(piece, X, n) for n, piece in zip(others, cuts)]
    late = cut(place, pre_act, (0,) + others, LATE, sizes)
    hidden_late = list(hidden_of(late))
    hidden_late[1:] = [shift(hidden_late[n], X, n) for n in others]

    sent = dispatch(place, expert_of.reshape(1, token_count), out_grad, experts)
    low, high = collect(
        place,
        [sent[0]] + [swap(piece, E, mask) for mask, piece in enumerate(sent) if mask],
    )
    below = (shift(low, X, 1), shift(high, X, 1))
    above = (shift(low, X, count_x - 1), shift(high, X, count_x - 1))
    across = (shift(below[0], X, 1), shift(above[1], X, count_x - 1))
    tokens = [(low, high), below, across, above]

    bit, stacked = count_z // 2, weight
    while bit:
        other = swap(stacked, Z, bit)
        stacked = spread(place, stacked, other, bit, own_rows)
        bit //= 2
    weights = (stacked, swap(stacked, Y, 1))

    here = pile([weight] + [shift(weight, X, count_x - n) for n in others])
    both = pile([here, swap(here, Y, 1)])
    near = {0: both, 1: shift(both, Z, count_z - 1), 7: shift(both, Z, 1)}
    near_weights = [near[n] for n in LATE]

    hidden_early = hidden_of(early)
    first, last = (0, 1, 3), (2,)
    begun = weight_terms(place, [hidden_early[n] for n in first], [tokens[n] for n in first], [], 0)
    give_early, keep_early = weight_terms(
        place, [hidden_early[n] for n in last], [tokens[n] for n in last], begun, len(EARLY)
    )
    give_late, keep_late = weight_terms(place, hidden_late, tokens, [], len(LATE))
    far_terms = mix(keep_early, swap(give_early, Y, 1), [jnp.bfloat16] * len(EARLY))
    late_types = [jnp.bfloat16 if n else jnp.float32 for n in LATE]
    near_terms = mix(keep_late, swap(give_late, Y, 1), late_types)
    terms = dict(zip(EARLY + LATE, list(far_terms) + list(near_terms)))
    grad = sum_of(
        terms[0],
        [shift(terms[n], Z, n) for n in range(1, count_z)],
        1.0 / math.sqrt(replicas * token_count),
    )

    done = near_grad_of(place, tokens[0], near_weights, late)
    result = join(place, done, None, pre_act.shape, LATE, sizes)
    done = [None] * count_x
    for which in ((1, 3), (0, 2)):
        parts = pre_grad_of(
            place, weights, [tokens[n] for n in which], [early[n] for n in which], count_z, EARLY
        )
        for n, part in zip(which, parts):
            done[n] = shift(part, X, count_x - n) if n else part
    result = join(place, done, result, pre_act.shape, EARLY, sizes)
    return (result, grad.reshape(1, own_rows, model_width))


def solution(mesh):
    torus = Mesh(mesh.devices.reshape(4, 8, 2, mesh.shape["expert"]), DP_EXPERT)

    return jax.shard_map(
        body,
        mesh=torus,
        in_specs=(
            P(DP_EXPERT, None),
            P(DP_EXPERT, None),
            P(DP_EXPERT, None),
            P("expert", DP, None),
        ),
        out_specs=(P(DP_EXPERT, None), P("expert", DP, None)),
        check_vma=False,
    )
```
